32 devices in a mesh: dp: 4 (over x, core), ep: 8 (over z, y).
Axes of the slice: x: 2, y: 2, z: 4, core: 2. Of those that a mesh axis runs over, the one named last changes fastest.
Arguments:
- tokens: bfloat16 [4096, 7168], P(('dp', 'ep')), may hold values from -6 to 6
- out_grad: bfloat16 [4096, 7168], P(('dp', 'ep')), may hold values from -3 to 3
- expert_ids: int32 [4096, 8], P(('dp', 'ep')), may hold values from 0 to 255, as said below
- route_weights: bfloat16 [4096, 8], P(('dp', 'ep')), may hold values from 0.099609375 to 1
- gate_matrix: bfloat16 [7168, 2048], P('dp', 'ep'), may hold values from -0.0625 to 0.0625
- up_matrix: bfloat16 [7168, 2048], P('dp', 'ep'), may hold values from -0.0625 to 0.0625
- down_matrix: bfloat16 [7168, 2048], P('dp', 'ep'), may hold values from -0.125 to 0.125
Outputs:
- input_gradient: bfloat16 [4096, 7168], P(('dp', 'ep'))
- route_gradient: float32 [4096, 8], P(('dp', 'ep'))
- gate_gradient: bfloat16 [7168, 2048], P('dp', 'ep')
- up_gradient: bfloat16 [7168, 2048], P('dp', 'ep')
- down_gradient: bfloat16 [7168, 2048], P('dp', 'ep')
The draws below stay inside these ranges and needn't reach their ends.
Inputs may be any that keep to these rules, and one draw needn't show every extreme that they name: `expert_ids`: each row names 8 different ids, 2 in each of 4 groups of 32 consecutive ids. In each aligned block of 1024 rows, one id that is a multiple of 256 is named by 8 or more rows of every aligned block of 128 rows inside it.
All inputs are finite; a program needn't handle non-finite values.
Results may differ from the reference program's by a relative error of at most 0.014.
Values may be sent and summed in bfloat16 or wider, within the bound.
A program may use at most 128 MiB of HBM per device.

```python
import math
import jax
import jax.numpy as jnp
from jax import lax

D = 7168
FF = 2048
ROUTED = 256
NGROUPS = 8
TOPG = 4
TOPK = 8
SLICES = 8
TOK_DEV = 128
HID_DEV = 256
EXPERTS = 1
STRIDE = 256
CAP = 8
TOKENS = 4096
N_DP = 4
N_EP = 8


def draw_expert_ids(key, part):
    total_rows = TOK_DEV * N_EP * N_DP
    group_width = ROUTED // NGROUPS
    per_group = TOPK // TOPG
    base = jax.random.fold_in(key, 7)
    key_hot = jax.random.fold_in(base, 1)
    key_groups = jax.random.fold_in(base, 2)
    key_members = jax.random.fold_in(base, 3)
    hottest = jax.random.randint(key_hot, (N_DP,), 0, EXPERTS) * STRIDE
    row_index = jnp.arange(total_rows, dtype=jnp.int32)
    forced = row_index % TOK_DEV < CAP
    hot_expert = hottest[row_index // (TOK_DEV * N_EP)]
    hot_group = hot_expert // group_width
    group_index = jnp.arange(NGROUPS, dtype=jnp.int32)
    group_scores = jax.random.randint(key_groups, (total_rows, NGROUPS), 0, 4096) * NGROUPS + group_index[None, :]
    group_scores = group_scores + jnp.where(forced[:, None] & (group_index[None, :] == hot_group[:, None]), 1 << 24, 0)
    chosen_groups = lax.top_k(group_scores, TOPG)[1].astype(jnp.int32)
    member_index = jnp.arange(group_width, dtype=jnp.int32)
    candidates = chosen_groups[:, :, None] * group_width + member_index[None, None, :]
    member_scores = jax.random.randint(key_members, (total_rows, TOPG, group_width), 0, 4096) * group_width + member_index[None, None, :]
    member_scores = member_scores + jnp.where(forced[:, None, None] & (candidates == hot_expert[:, None, None]), 1 << 24, 0)
    picked = lax.top_k(member_scores, per_group)[1]
    chosen = jnp.take_along_axis(candidates, picked, axis=2)
    return chosen.reshape(total_rows, TOPK).astype(jnp.int32)


def levels(rng, extent, cuts, smallest, high):
    factor_of, own = 1.0, jax.random.fold_in(rng, 6)
    for axis_at, parts in cuts:
        steps = jnp.exp(jax.random.uniform(jax.random.fold_in(own, axis_at), (parts,), jnp.float32, smallest / len(cuts), high / len(cuts)))
        factor_of = factor_of * jnp.repeat(steps, extent[axis_at] // parts).reshape([-1 if axis == axis_at else 1 for axis in range(len(extent))])
    return factor_of


def noise(key, shape, spread, reach, shards=(), kind=jnp.bfloat16):
    values = spread * jax.random.normal(key, shape, jnp.float32)
    if shards:
        values = values * levels(key, shape, shards, -0.22, 0.18)
    return jnp.clip(values, -reach, reach).astype(kind)


def setup_inputs(seed: int = 0) -> dict:
    keys = jax.random.split(jax.random.key(seed), 8)
    return {
        "tokens": noise(keys[0], (TOKENS, D), 1.0, 6.0, ((0, 32),)),
        "out_grad": noise(keys[1], (TOKENS, D), 0.5, 3.0, ((0, 32),)),
        "expert_ids": draw_expert_ids(jax.random.fold_in(keys[7], 71), 0),
        "route_weights": jnp.clip(jnp.exp(math.log(1.0) - 2.306499 * jax.random.uniform(keys[3], (TOKENS, TOPK), jnp.float32) ** levels(keys[3], (TOKENS, TOPK), ((0, 32),), -0.2, 0.2)), 0.099609375, 1.0).astype(jnp.bfloat16),
        "gate_matrix": noise(keys[4], (D, EXPERTS * FF), D ** -0.5, 0.0625, ((0, 4), (1, 8))),
        "up_matrix": noise(keys[5], (D, EXPERTS * FF), D ** -0.5, 0.0625, ((0, 4), (1, 8))),
        "down_matrix": noise(keys[6], (D, EXPERTS * FF), FF ** -0.5, 0.125, ((0, 4), (1, 8))),
    }


def assignments(expert_ids):
    blocks = expert_ids.shape[0] // TOK_DEV
    flat_ids = expert_ids.reshape(blocks, TOK_DEV * TOPK)
    window = (flat_ids % STRIDE) == 0
    expert = jnp.where(window, flat_ids // STRIDE, EXPERTS).astype(jnp.int32)
    column = jnp.arange(EXPERTS, dtype=jnp.int32)
    onehot = (expert[:, :, None] == column[None, None, :]).astype(jnp.int32)
    earlier = jnp.cumsum(onehot, axis=1) - onehot
    slot_index = jnp.sum(earlier * onehot, axis=2)
    kept_entry = window & (slot_index < CAP)
    target = expert * CAP + slot_index
    places = jnp.arange(EXPERTS * CAP, dtype=jnp.int32)
    table = kept_entry[:, :, None] & (target[:, :, None] == places[None, None, :])
    return table.reshape(blocks, TOK_DEV, TOPK, EXPERTS * CAP).astype(jnp.float32)


def widen(values):
    return lax.optimization_barrier(values.astype(jnp.bfloat16)).astype(jnp.float32)


def reference(tokens, out_grad, expert_ids, route_weights, gate_matrix, up_matrix, down_matrix):
    table = assignments(expert_ids)
    blocks = table.shape[0]
    select = jnp.sum(table, axis=2)
    select_half = select.astype(jnp.bfloat16)

    def dispatch_block(arguments):
        choose, block_in, block_grad = arguments
        first = jnp.dot(choose.T, block_in, preferred_element_type=jnp.float32).astype(jnp.bfloat16)
        second = jnp.dot(choose.T, block_grad, preferred_element_type=jnp.float32).astype(jnp.bfloat16)
        return first, second

    slot_in, slot_grad = lax.map(dispatch_block, (select_half, tokens.reshape(blocks, TOK_DEV, D), out_grad.reshape(blocks, TOK_DEV, D)))
    slot_gate = jnp.einsum("btks,btk->bs", table, route_weights.astype(jnp.float32).reshape(blocks, TOK_DEV, TOPK), precision=lax.Precision.HIGHEST).astype(jnp.bfloat16)

    def arrange(values):
        shaped = values.reshape((N_DP, N_EP, EXPERTS, CAP) + values.shape[2:])
        moved = jnp.moveaxis(shaped, 2, 0)
        return moved.reshape((EXPERTS, N_DP, N_EP * CAP) + values.shape[2:])

    def unarrange(values):
        shaped = values.reshape((EXPERTS, N_DP, N_EP, CAP) + values.shape[3:])
        moved = jnp.moveaxis(shaped, 0, 2)
        return moved.reshape((blocks, EXPERTS * CAP) + values.shape[3:])

    def expert_backward(arguments):
        rows_in, rows_grad, rows_gate, expert = arguments
        begin = (expert * FF).astype(jnp.int32)
        gate_cols = lax.dynamic_slice_in_dim(gate_matrix, begin, FF, 1)
        up_cols = lax.dynamic_slice_in_dim(up_matrix, begin, FF, 1)
        down_cols = lax.dynamic_slice_in_dim(down_matrix, begin, FF, 1)

        def one_group(total, group_arguments):
            group_in, group_grad, group_gate = group_arguments
            row_count = group_in.shape[0]
            gate_pre = jnp.dot(group_in, gate_cols, preferred_element_type=jnp.float32)
            up_pre = jnp.dot(group_in, up_cols, preferred_element_type=jnp.float32)
            projected = jnp.dot(group_grad, down_cols, preferred_element_type=jnp.float32)
            sigmoid = jax.nn.sigmoid(gate_pre)
            swished = gate_pre * sigmoid
            hidden = widen(swished * up_pre)
            slice_sums = jnp.sum((hidden * projected).reshape(row_count, SLICES, HID_DEV), axis=2)
            route_part = jnp.sum(widen(slice_sums), axis=1)
            scaling = group_gate.astype(jnp.float32)[:, None]
            grad_hidden = scaling * projected
            gate_delta = (grad_hidden * up_pre * sigmoid * (1.0 + gate_pre * (1.0 - sigmoid))).astype(jnp.bfloat16)
            up_delta = (grad_hidden * swished).astype(jnp.bfloat16)
            scaled = (scaling * hidden).astype(jnp.bfloat16)
            partial_value = jnp.zeros((row_count, D), jnp.float32)
            for piece in range(SLICES):
                low = piece * HID_DEV
                high = low + HID_DEV
                term = jnp.dot(gate_delta[:, low:high], gate_cols[:, low:high].T, preferred_element_type=jnp.float32)
                term = term + jnp.dot(up_delta[:, low:high], up_cols[:, low:high].T, preferred_element_type=jnp.float32)
                partial_value = partial_value + widen(term)
            grads = jnp.concatenate([
                jnp.dot(group_in.T, gate_delta, preferred_element_type=jnp.float32),
                jnp.dot(group_in.T, up_delta, preferred_element_type=jnp.float32),
                jnp.dot(group_grad.T, scaled, preferred_element_type=jnp.float32)], axis=1)
            total = total + widen(grads)
            return total, (partial_value, route_part)

        start_total = jnp.zeros((D, 3 * FF), jnp.float32)
        total, outputs = lax.scan(one_group, start_total, (rows_in, rows_grad, rows_gate))
        return total.astype(jnp.bfloat16), outputs[0], outputs[1]

    totals, partials, route_parts = lax.map(expert_backward, (arrange(slot_in), arrange(slot_grad), arrange(slot_gate), jnp.arange(EXPERTS, dtype=jnp.int32)))
    slot_partial = unarrange(partials)
    slot_route = unarrange(route_parts)

    def combine_block(arguments):
        choose, values = arguments
        return jnp.dot(choose, values, precision=lax.Precision.HIGHEST).astype(jnp.bfloat16)

    input_gradient = lax.map(combine_block, (select, slot_partial)).reshape(blocks * TOK_DEV, D)
    route_gradient = jnp.einsum("btks,bs->btk", table, slot_route, precision=lax.Precision.HIGHEST).reshape(blocks * TOK_DEV, TOPK)
    gate_gradient = jnp.moveaxis(totals[:, :, :FF], 0, 1).reshape(D, EXPERTS * FF)
    up_gradient = jnp.moveaxis(totals[:, :, FF:2 * FF], 0, 1).reshape(D, EXPERTS * FF)
    down_gradient = jnp.moveaxis(totals[:, :, 2 * FF:], 0, 1).reshape(D, EXPERTS * FF)
    return (input_gradient, route_gradient, gate_gradient, up_gradient, down_gradient)
```

```python
import functools
import jax
import jax.numpy as jnp
from jax import lax
from jax.experimental import pallas as pl
from jax.experimental.pallas import tpu as pltpu
from jax.sharding import PartitionSpec as P

ROUTED = 256
TOPK = 8
SLICES = 8
CAP = 8
LANES = 128
BF = jnp.bfloat16
F32 = jnp.float32
MESH = pl.DeviceIdType.MESH


def kernel(
    n_dp, n_ep,
    tok_hbm, grad_hbm, ids_ref, rw_ref, a_hbm, b_hbm, c_hbm,
    ig_hbm, rg_ref, ga_hbm, gb_hbm, gc_hbm,
    tokbuf, gradbuf, wab, wc, send1, shard, ag, xs, ys, gates, psum, arsend, arrecv,
    deltas, scaleds, rp, r1recv, r2send, r2recv, retbuf, fin, ga, gb, gc,
    in_sem, w_sem, out_sem, s1s, s1r, s2s, s2r, s3s, s3r, ars, arr, r1s, r1r, r2s, r2r, fs, fr,
):
    experts = n_ep // SLICES
    stride = ROUTED // experts
    places = experts * CAP
    n_hi = n_ep // 2
    rows, width = tok_hbm.shape
    lw, hid = a_hbm.shape
    nb = n_dp.bit_length() - 1
    chunk = 2 * n_dp * CAP
    half = n_dp * CAP
    g = lax.axis_index("dp")
    e = lax.axis_index("ep")
    hi, lo = e // 2, e % 2
    other = hi * 2 + (1 - lo)
    mine_w = e // SLICES

    def rc(src, dst, ss, rs, **where):
        return pltpu.make_async_remote_copy(
            src_ref=src, dst_ref=dst, send_sem=ss, recv_sem=rs,
            device_id=where, device_id_type=MESH)

    def cols(j):
        gp = lax.rem(g + j, n_dp)
        return gp, pl.ds(pl.multiple_of(gp * lw, LANES), lw)

    loads = []
    order = list(range(1, n_dp)) + [0]
    for j in order:
        gp, ds = cols(j)
        c1 = pltpu.make_async_copy(tok_hbm.at[:, ds], tokbuf.at[j], in_sem.at[0, j])
        c2 = pltpu.make_async_copy(grad_hbm.at[:, ds], gradbuf.at[j], in_sem.at[1, j])
        c1.start()
        c2.start()
        loads.append((j, gp, c1, c2))
    wloads = [
        pltpu.make_async_copy(a_hbm, wab.at[:, pl.ds(0, hid)], w_sem.at[0]),
        pltpu.make_async_copy(b_hbm, wab.at[:, pl.ds(hid, hid)], w_sem.at[1]),
        pltpu.make_async_copy(c_hbm, wc, w_sem.at[2]),
    ]
    for c in wloads:
        c.start()

    barrier = pltpu.get_barrier_semaphore()
    for j in range(1, n_dp):
        pl.semaphore_signal(barrier, inc=1, device_id={"dp": lax.rem(g + j, n_dp)}, device_id_type=MESH)
    for j in range(1, n_hi):
        pl.semaphore_signal(
            barrier, inc=1, device_id={"ep": lax.rem(hi + j, n_hi) * 2 + lo}, device_id_type=MESH)
    pl.semaphore_signal(barrier, inc=1, device_id={"ep": other}, device_id_type=MESH)

    ids = ids_ref[...]
    rw = rw_ref[...].astype(F32)
    lane = lax.broadcasted_iota(jnp.int32, (rows, LANES), 1)
    wanted = jnp.where(lane < places, (lane // CAP) * stride, -1)
    hits = jnp.zeros((rows, LANES), F32)
    wts = jnp.zeros((rows, LANES), F32)
    for k in range(TOPK):
        m = ids[:, k:k + 1] == wanted
        hits = hits + jnp.where(m, 1.0, 0.0)
        wts = wts + jnp.where(m, rw[:, k:k + 1], 0.0)
    tr = lax.broadcasted_iota(jnp.int32, (rows, rows), 0)
    tc = lax.broadcasted_iota(jnp.int32, (rows, rows), 1)
    lower = jnp.where(tc < tr, 1.0, 0.0).astype(BF)
    slot = jnp.dot(lower, hits.astype(BF), preferred_element_type=F32)
    sel = jnp.where(slot == (lane % CAP).astype(F32), hits, 0.0)
    selT = sel.T[:places].astype(BF)
    gwT = (sel * wts).T[:places].astype(BF)
    gate = jnp.dot(gwT, jnp.ones((rows, LANES), BF), preferred_element_type=F32)
    gate = gate.reshape(experts, CAP, LANES).astype(BF)

    pl.semaphore_wait(barrier, n_dp - 1 + n_hi)

    for j, gp, c1, c2 in loads:
        c1.wait()
        c2.wait()
        xr = jnp.dot(selT, tokbuf[j], preferred_element_type=F32).reshape(experts, CAP, lw).astype(BF)
        yr = jnp.dot(selT, gradbuf[j], preferred_element_type=F32).reshape(experts, CAP, lw).astype(BF)
        if j:
            send1[j, :, :, 0:lw] = xr
            send1[j, :, :, lw:2 * lw] = yr
            send1[j, :, :, 2 * lw:] = gate
            rc(send1.at[j], shard.at[:, g], s1s.at[j], s1r.at[g], dp=gp).start()
        else:
            shard[:, g, :, 0:lw] = xr
            shard[:, g, :, lw:2 * lw] = yr
            shard[:, g, :, 2 * lw:] = gate
    for j in range(1, n_dp):
        src = lax.rem(g + j, n_dp)
        rc(send1.at[j], shard.at[:, src], s1s.at[j], s1r.at[src], dp=src).wait_recv()

    def hop(i):
        h = lax.rem(hi + i, n_hi)
        return rc(shard.at[(h * 2) // SLICES], ag.at[e], s2s.at[h], s2r.at[hi], ep=h * 2 + lo)

    def hop_in(h):
        return rc(shard.at[0], ag.at[h * 2 + lo], s2s.at[h], s2r.at[h], ep=other)

    def fwd(h):
        return rc(ag.at[h * 2 + lo], ag.at[h * 2 + lo], s3s.at[h], s3r.at[h], ep=other)

    def fwd_in(h):
        return rc(ag.at[h * 2 + 1 - lo], ag.at[h * 2 + 1 - lo], s3s.at[h], s3r.at[h], ep=other)

    rc(shard.at[mine_w], ag.at[e], s3s.at[hi], s3r.at[hi], ep=other).start()
    for i in range(1, n_hi):
        hop(i).start()
    ag[e] = shard[mine_w]
    for c in wloads:
        c.wait()

    def ar(b, h):
        bit = 1 << b
        peer = g + (1 - 2 * ((g // bit) % 2)) * bit
        return rc(arsend.at[b, h], arrecv.at[b, h], ars.at[b, h], arr.at[b, h], dp=peer)

    def at_chunk(h):
        return pl.ds(pl.multiple_of(h * chunk, 16), chunk)

    def flow(i, carry):
        @pl.when((i >= 1) & (i < n_hi))
        def _():
            h = lax.rem(hi + i, n_hi)
            hop_in(h).wait_recv()
            fwd(h).start()

        @pl.when((i >= 1) & (i <= n_hi))
        def _():
            h = lax.rem(hi + i - 1, n_hi)
            fwd_in(h).wait_recv()
            got = ag.at[pl.ds(h * 2, 2)]
            x = got[:, :, :, 0:lw].astype(F32).reshape(chunk, lw).astype(BF)
            y = got[:, :, :, lw:2 * lw].astype(F32).reshape(chunk, lw).astype(BF)
            gates[at_chunk(h), :] = got[:, :, :, 2 * lw:].astype(F32).reshape(chunk, LANES)
            xs[at_chunk(h), :] = x
            ys[at_chunk(h), :] = y
            p1 = jnp.dot(x, wab[...], preferred_element_type=F32)
            p2 = jnp.dot(y, wc[...], preferred_element_type=F32)
            psum[h, :, 0:2 * hid] = p1
            psum[h, :, 2 * hid:] = p2
            arsend[0, h, :, 0:2 * hid] = p1.astype(BF)
            arsend[0, h, :, 2 * hid:] = p2.astype(BF)
            ar(0, h).start()

        for b in range(nb - 1):
            @pl.when((i >= 2 + b) & (i < n_hi + 2 + b))
            def _(b=b):
                h = lax.rem(hi + i - 2 - b, n_hi)
                ar(b, h).wait_recv()
                s = psum[h] + arrecv[b, h].astype(F32)
                psum[h] = s
                arsend[b + 1, h] = s.astype(BF)
                ar(b + 1, h).start()
        return carry

    lax.fori_loop(0, n_hi + nb, flow, 0)

    def r1(h):
        return rc(rp.at[h, 1 - lo], r1recv.at[h], r1s.at[h], r1r.at[h], ep=other)

    def finish(i, carry):
        h = lax.rem(hi + i + 1, n_hi)
        ar(nb - 1, h).wait_recv()
        s = psum[h] + arrecv[nb - 1, h].astype(F32)
        gate_pre, up_pre, proj = s[:, :hid], s[:, hid:2 * hid], s[:, 2 * hid:]
        scaling = gates[at_chunk(h), 0:1]
        sig = 1.0 / (1.0 + jnp.exp(-gate_pre))
        sw = gate_pre * sig
        hidden = (sw * up_pre).astype(BF).astype(F32)
        route = jnp.sum(hidden * proj, axis=1, keepdims=True)
        gh = scaling * proj
        d1 = (gh * up_pre * sig * (1.0 + gate_pre * (1.0 - sig))).astype(BF)
        d2 = (gh * sw).astype(BF)
        deltas[at_chunk(h), 0:hid] = d1
        deltas[at_chunk(h), hid:] = d2
        scaleds[at_chunk(h), :] = (scaling * hidden).astype(BF)
        part = lax.dot_general(
            jnp.concatenate([d1, d2], axis=1), wab[...], (((1,), (1,)), ((), ())),
            preferred_element_type=F32)
        rp[h, :, :, 0:lw] = part.reshape(2, half, lw).astype(BF)
        rp[h, :, :, lw:] = jnp.broadcast_to(route, (chunk, LANES)).reshape(2, half, LANES).astype(BF)
        r1(h).start()
        return carry

    lax.fori_loop(0, n_hi, finish, 0)

    def r2(h):
        return rc(r2send.at[h], r2recv.at[hi], r2s.at[h], r2r.at[hi], ep=h * 2 + lo)

    def pair(h):
        r1(h).wait_recv()
        return rp[h, lo].astype(F32) + r1recv[h].astype(F32)

    def combine(i, carry):
        h = lax.rem(hi + i, n_hi)
        r2send[h] = pair(h).astype(BF)
        r2(h).start()
        return carry

    lax.fori_loop(1, n_hi, combine, 0)
    r2recv[hi] = pair(hi).astype(BF)

    tile = 256 if lw % 256 == 0 else 128

    def wgrad(i, carry):
        ds = pl.ds(pl.multiple_of(i * tile, LANES), tile)
        dn = (((0,), (0,)), ((), ()))
        both = lax.dot_general(xs[:, ds], deltas[...], dn, preferred_element_type=F32).astype(BF)
        ga[ds, :] = both[:, :hid]
        gb[ds, :] = both[:, hid:]
        gc[ds, :] = lax.dot_general(ys[:, ds], scaleds[...], dn, preferred_element_type=F32).astype(BF)
        return carry

    lax.fori_loop(0, lw // tile, wgrad, 0)
    outs = [
        pltpu.make_async_copy(ga, ga_hbm, w_sem.at[0]),
        pltpu.make_async_copy(gb, gb_hbm, w_sem.at[1]),
        pltpu.make_async_copy(gc, gc_hbm, w_sem.at[2]),
    ]
    for c in outs:
        c.start()

    for i in range(1, n_hi):
        h = lax.rem(hi + i, n_hi)
        rc(r2send.at[h], r2recv.at[h], r2s.at[h], r2r.at[h], ep=h * 2 + lo).wait_recv()
    per = SLICES // 2
    for w in range(experts):
        acc = r2recv[w * per].astype(F32)
        for j in range(1, per):
            acc = acc + r2recv[w * per + j].astype(F32)
        retbuf[:, w] = acc.reshape(n_dp, CAP, lw + LANES).astype(BF)
    for j in range(1, n_dp):
        gp = lax.rem(g + j, n_dp)
        rc(retbuf.at[gp], fin.at[g], fs.at[j], fr.at[g], dp=gp).start()
    fin[g] = retbuf[g]
    selP = sel[:, :places].astype(BF)
    ocopies = []
    for j in range(n_dp):
        gp, ds = cols(j)
        if j:
            rc(retbuf.at[gp], fin.at[gp], fs.at[j], fr.at[gp], dp=gp).wait_recv()
        vals = fin[gp].astype(F32).reshape(places, lw + LANES)
        if j == 0:
            route = jnp.concatenate(
                [vals[:, lw:], jnp.zeros((LANES - places, LANES), F32)], axis=0).T[0:1]
            lane8 = lax.broadcasted_iota(jnp.int32, (rows, TOPK), 1)
            rg = jnp.zeros((rows, TOPK), F32)
            terms = sel * route
            for k in range(TOPK):
                v = jnp.sum(jnp.where(ids[:, k:k + 1] == wanted, terms, 0.0), axis=1, keepdims=True)
                rg = jnp.where(lane8 == k, v, rg)
            rg_ref[...] = rg
        tokbuf[j] = jnp.dot(selP, vals[:, :lw].astype(BF), preferred_element_type=F32).astype(BF)
        c = pltpu.make_async_copy(tokbuf.at[j], ig_hbm.at[:, ds], out_sem.at[j])
        c.start()
        ocopies.append(c)

    for j in range(1, n_dp):
        gp = lax.rem(g + j, n_dp)
        rc(send1.at[j], shard.at[:, g], s1s.at[j], s1r.at[g], dp=gp).wait_send()
        rc(retbuf.at[gp], fin.at[g], fs.at[j], fr.at[g], dp=gp).wait_send()

    def drain(i, carry):
        h = lax.rem(hi + i, n_hi)
        fwd(h).wait_send()
        for b in range(nb):
            ar(b, h).wait_send()
        r1(h).wait_send()

        @pl.when(i >= 1)
        def _():
            hop(i).wait_send()
            r2(h).wait_send()
        return carry

    lax.fori_loop(0, n_hi, drain, 0)
    for c in outs + ocopies:
        c.wait()


def body(tokens, out_grad, expert_ids, route_weights, gate_matrix, up_matrix, down_matrix):
    n_dp, n_ep = lax.axis_size("dp"), lax.axis_size("ep")
    experts = n_ep // SLICES
    n_hi = n_ep // 2
    rows, width = tokens.shape
    lw, hid = gate_matrix.shape
    nb = n_dp.bit_length() - 1
    chunk = 2 * n_dp * CAP
    half = n_dp * CAP
    total = n_hi * chunk
    C = 2 * lw + LANES
    R = lw + LANES
    V = pltpu.VMEM
    D = lambda *s: pltpu.SemaphoreType.DMA(s)
    anyspec = pl.BlockSpec(memory_space=pl.ANY)
    vspec = pl.BlockSpec(memory_space=pltpu.VMEM)
    return pl.pallas_call(
        functools.partial(kernel, n_dp, n_ep),
        out_shape=(
            jax.ShapeDtypeStruct((rows, width), BF),
            jax.ShapeDtypeStruct((rows, TOPK), F32),
            jax.ShapeDtypeStruct((lw, hid), BF),
            jax.ShapeDtypeStruct((lw, hid), BF),
            jax.ShapeDtypeStruct((lw, hid), BF),
        ),
        in_specs=[anyspec, anyspec, vspec, vspec, anyspec, anyspec, anyspec],
        out_specs=(anyspec, vspec, anyspec, anyspec, anyspec),
        scratch_shapes=[
            V((n_dp, rows, lw), BF), V((n_dp, rows, lw), BF), V((lw, 2 * hid), BF), V((lw, hid), BF),
            V((n_dp, experts, CAP, C), BF), V((experts, n_dp, CAP, C), BF), V((n_ep, n_dp, CAP, C), BF),
            V((total, lw), BF), V((total, lw), BF), V((total, LANES), F32),
            V((n_hi, chunk, 3 * hid), F32), V((nb, n_hi, chunk, 3 * hid), BF), V((nb, n_hi, chunk, 3 * hid), BF),
            V((total, 2 * hid), BF), V((total, hid), BF),
            V((n_hi, 2, half, R), BF), V((n_hi, half, R), BF), V((n_hi, half, R), BF), V((n_hi, half, R), BF),
            V((n_dp, experts, CAP, R), BF), V((n_dp, experts, CAP, R), BF),
            V((lw, hid), BF), V((lw, hid), BF), V((lw, hid), BF),
            D(2, n_dp), D(3), D(n_dp), D(n_dp), D(n_dp), D(n_hi), D(n_hi), D(n_hi), D(n_hi),
            D(nb, n_hi), D(nb, n_hi), D(n_hi), D(n_hi), D(n_hi), D(n_hi), D(n_dp), D(n_dp),
        ],
        compiler_params=pltpu.CompilerParams(
            collective_id=0, has_side_effects=True, vmem_limit_bytes=67043328),
    )(tokens, out_grad, expert_ids, route_weights, gate_matrix, up_matrix, down_matrix)


def solution(mesh):
    return jax.shard_map(
        body,
        mesh=mesh,
        in_specs=(
            P(("dp", "ep"), None),
            P(("dp", "ep"), None),
            P(("dp", "ep"), None),
            P(("dp", "ep"), None),
            P("dp", "ep"),
            P("dp", "ep"),
            P("dp", "ep"),
        ),
        out_specs=(
            P(("dp", "ep"), None),
            P(("dp", "ep"), None),
            P("dp", "ep"),
            P("dp", "ep"),
            P("dp", "ep"),
        ),
        check_vma=False,
    )
```

```python
import functools
import jax
import jax.numpy as jnp
from jax import lax
from jax.experimental import pallas as pl
from jax.experimental.pallas import tpu as pltpu
from jax.sharding import PartitionSpec as P

ROUTED = 256
TOPK = 8
SLICES = 8
CAP = 8
LANES = 128
BF = jnp.bfloat16
F32 = jnp.float32
MESH = pl.DeviceIdType.MESH


def kernel(
    n_dp, n_ep,
    tok_hbm, grad_hbm, ids_ref, rw_ref, a_hbm, b_hbm, c_hbm,
    fin, sel_ref, ga_hbm, gb_hbm, gc_hbm,
    tokbuf, gradbuf, wab, wc, send1, shard, ag, xs, ys, gates, psum, arsend, arrecv,
    deltas, scaleds, rp, r1recv, r2send, r2recv, retbuf, ga, gb, gc,
    in_sem, w_sem, s1s, s1r, s2s, s2d, s2r, sas, s3s, s3r, ars, arr, r1s, r1r, r2s, r2r, fs, fr,
):
    experts = n_ep // SLICES
    stride = ROUTED // experts
    places = experts * CAP
    n_hi = n_ep // 2
    rows, width = tok_hbm.shape
    lw, hid = a_hbm.shape
    nb = n_dp.bit_length() - 1
    chunk = 2 * n_dp * CAP
    half = n_dp * CAP
    g = lax.axis_index("dp")
    e = lax.axis_index("ep")
    hi, lo = e // 2, e % 2
    other = hi * 2 + (1 - lo)
    mine_w = e // SLICES

    def rc(src, dst, ss, rs, **where):
        return pltpu.make_async_remote_copy(
            src_ref=src, dst_ref=dst, send_sem=ss, recv_sem=rs,
            device_id=where, device_id_type=MESH)

    def cols(j):
        gp = lax.rem(g + j, n_dp)
        return gp, pl.ds(pl.multiple_of(gp * lw, LANES), lw)

    order = [n_dp // 2] + [j for j in range(1, n_dp) if j != n_dp // 2] + [0]
    loads = []
    for q, (src, buf) in enumerate(((tok_hbm, tokbuf), (grad_hbm, gradbuf))):
        for j in order:
            gp, ds = cols(j)
            c = pltpu.make_async_copy(src.at[:, ds], buf.at[j], in_sem.at[q, j])
            c.start()
            loads.append((q, j, gp, buf, c))
    wloads = [
        pltpu.make_async_copy(a_hbm, wab.at[:, pl.ds(0, hid)], w_sem.at[0]),
        pltpu.make_async_copy(b_hbm, wab.at[:, pl.ds(hid, hid)], w_sem.at[1]),
        pltpu.make_async_copy(c_hbm, wc, w_sem.at[2]),
    ]

    barrier = pltpu.get_barrier_semaphore()
    for j in range(1, n_dp):
        pl.semaphore_signal(barrier, inc=1, device_id={"dp": lax.rem(g + j, n_dp)}, device_id_type=MESH)
    for j in range(1, n_hi):
        pl.semaphore_signal(
            barrier, inc=1, device_id={"ep": lax.rem(hi + j, n_hi) * 2 + lo}, device_id_type=MESH)
    pl.semaphore_signal(barrier, inc=1, device_id={"ep": other}, device_id_type=MESH)

    pad = jnp.zeros((LANES - TOPK, rows), F32)
    ids = jnp.concatenate([ids_ref[...].astype(F32), pad], axis=0).T
    rw = jnp.concatenate([rw_ref[...].astype(F32), pad], axis=0).T
    lane = lax.broadcasted_iota(jnp.int32, (rows, LANES), 1)
    wanted = jnp.where(lane < places, (lane // CAP) * stride, -1).astype(F32)
    hits = jnp.zeros((rows, LANES), F32)
    wts = jnp.zeros((rows, LANES), F32)
    for k in range(TOPK):
        m = ids[:, k:k + 1] == wanted
        hits = hits + jnp.where(m, 1.0, 0.0)
        wts = wts + jnp.where(m, rw[:, k:k + 1], 0.0)
    tr = lax.broadcasted_iota(jnp.int32, (rows, rows), 0)
    tc = lax.broadcasted_iota(jnp.int32, (rows, rows), 1)
    lower = jnp.where(tc < tr, 1.0, 0.0).astype(BF)
    slot = jnp.dot(lower, hits.astype(BF), preferred_element_type=F32)
    sel = jnp.where(slot == (lane % CAP).astype(F32), hits, 0.0)
    sel_ref[...] = sel
    selT = sel.T[:places].astype(BF)
    gwT = (sel * wts).T[:places].astype(BF)
    gate = jnp.dot(gwT, jnp.ones((rows, LANES), BF), preferred_element_type=F32)
    gate = gate.reshape(experts, CAP, LANES).astype(BF)

    pl.semaphore_wait(barrier, n_dp - 1 + n_hi)

    pieces = (pl.ds(0, lw), pl.ds(lw, lw + LANES))

    def slices(j, q, gp):
        return rc(send1.at[j, :, :, pieces[q]], shard.at[:, g, :, pieces[q]], s1s.at[q, j], s1r.at[q, g], dp=gp)

    for q, j, gp, buf, c in loads:
        c.wait()
        r = jnp.dot(selT, buf[j], preferred_element_type=F32).reshape(experts, CAP, lw).astype(BF)
        if j:
            send1[j, :, :, q * lw:(q + 1) * lw] = r
            if q:
                send1[j, :, :, 2 * lw:] = gate
            slices(j, q, gp).start()
        else:
            shard[:, g, :, q * lw:(q + 1) * lw] = r
            if q:
                shard[:, g, :, 2 * lw:] = gate
    for c in wloads:
        c.start()

    per = SLICES // 2
    pos = hi % per
    base = hi - pos

    def at_order(k):
        m = jnp.where(pos < per - 1 - pos, pos, per - 1 - pos)
        near = jnp.where(k % 2 == 1, pos - (k + 1) // 2, pos + k // 2)
        far = jnp.where(pos < per - 1 - pos, k, per - 1 - k)
        return jnp.where(k <= 2 * m, near, far)

    def seen(h, q):
        return ag.at[h * 2 + lo, :, :, pieces[q]]

    def link(p, v, q, up):
        h = v * per + p
        to = hi + 1 - 2 * up
        return rc(seen(h, q), seen(h, q), (s2d if up else s2s).at[h, q], s2r.at[h, q], ep=to * 2 + lo)

    def link_in(p, v, q):
        h = v * per + p
        return rc(seen(h, q), seen(h, q), s2s.at[h, q], s2r.at[h, q], ep=other)

    def fwd(p, v, q):
        h = v * per + p
        return rc(seen(h, q), seen(h, q), s3s.at[h, q], s3r.at[h, q], ep=other)

    def fwd_in(p, v, q):
        h = v * per + p
        r = ag.at[h * 2 + 1 - lo, :, :, pieces[q]]
        return rc(r, r, s3s.at[h, q], s3r.at[h, q], ep=other)

    def across(i, q):
        h = lax.rem(hi + i * per, n_hi)
        return rc(shard.at[h // per, :, :, pieces[q]], seen(hi, q), sas.at[i, q], s2r.at[hi, q], ep=h * 2 + lo)

    def across_in(i, q):
        h = lax.rem(hi + i * per, n_hi)
        return rc(seen(h, q), seen(h, q), sas.at[i, q], s2r.at[h, q], ep=other)

    def onward(p, v, q, wait):
        @pl.when((p <= pos) & (pos < per - 1))
        def _():
            d = link(p, v, q, 0)
            d.wait_send() if wait else d.start()

        @pl.when((p >= pos) & (pos > 0))
        def _():
            d = link(p, v, q, 1)
            d.wait_send() if wait else d.start()

    for q in range(2):
        for j in range(1, n_dp):
            src = lax.rem(g + j, n_dp)
            rc(send1.at[j, :, :, pieces[q]], shard.at[:, src, :, pieces[q]], s1s.at[q, j], s1r.at[q, src], dp=src).wait_recv()
        for i in range(1, experts):
            across(i, q).start()
        if q:
            ag[e, :, :, lw:] = shard[mine_w, :, :, lw:]
        else:
            ag[e, :, :, :lw] = shard[mine_w, :, :, :lw]
        onward(pos, mine_w, q, False)
        fwd(pos, mine_w, q).start()
        for i in range(1, experts):
            across_in(i, q).wait_recv()
            v = lax.rem(mine_w + i, experts)
            onward(pos, v, q, False)
            fwd(pos, v, q).start()
    for c in wloads:
        c.wait()

    def ar(b, h):
        bit = 1 << b
        peer = g + (1 - 2 * ((g // bit) % 2)) * bit
        return rc(arsend.at[b, h], arrecv.at[b, h], ars.at[b, h], arr.at[b, h], dp=peer)

    def at_chunk(h):
        return pl.ds(pl.multiple_of(h * chunk, 16), chunk)

    def chunk_of(t):
        p, v = at_order(t // experts), t % experts
        return p, v, v * per + p

    def flow(t, carry):
        @pl.when((t >= experts) & (t < n_hi))
        def _():
            p, v, h = chunk_of(t)
            for q in range(2):
                link_in(p, v, q).wait_recv()
                onward(p, v, q, False)
                fwd(p, v, q).start()

        @pl.when((t >= 1) & (t <= n_hi))
        def _():
            p, v, h = chunk_of(t - 1)
            fwd_in(p, v, 0).wait_recv()
            x = ag[pl.ds(h * 2, 2), :, :, 0:lw].astype(F32).reshape(chunk, lw).astype(BF)
            xs[at_chunk(h), :] = x
            p1 = jnp.dot(x, wab[...], preferred_element_type=F32)
            psum[h, :, 0:2 * hid] = p1
            arsend[0, h, :, 0:2 * hid] = p1.astype(BF)
            fwd_in(p, v, 1).wait_recv()
            y = ag[pl.ds(h * 2, 2), :, :, lw:2 * lw].astype(F32).reshape(chunk, lw).astype(BF)
            gates[at_chunk(h), :] = ag[pl.ds(h * 2, 2), :, :, 2 * lw:].astype(F32).reshape(chunk, LANES)
            ys[at_chunk(h), :] = y
            p2 = jnp.dot(y, wc[...], preferred_element_type=F32)
            psum[h, :, 2 * hid:] = p2
            arsend[0, h, :, 2 * hid:] = p2.astype(BF)
            ar(0, h).start()

        for b in range(nb - 1):
            @pl.when((t >= 2 + b) & (t < n_hi + 2 + b))
            def _(b=b):
                p, v, h = chunk_of(t - 2 - b)
                ar(b, h).wait_recv()
                s = psum[h] + arrecv[b, h].astype(F32)
                psum[h] = s
                arsend[b + 1, h] = s.astype(BF)
                ar(b + 1, h).start()
        return carry

    lax.fori_loop(0, n_hi + nb, flow, 0)

    def r1(h):
        return rc(rp.at[h, 1 - lo], r1recv.at[h], r1s.at[h], r1r.at[h], ep=other)

    def finish(i, carry):
        p, v, h = chunk_of(i)
        ar(nb - 1, h).wait_recv()
        s = psum[h] + arrecv[nb - 1, h].astype(F32)
        gate_pre, up_pre, proj = s[:, :hid], s[:, hid:2 * hid], s[:, 2 * hid:]
        scaling = gates[at_chunk(h), 0:1]
        sig = 1.0 / (1.0 + jnp.exp(-gate_pre))
        sw = gate_pre * sig
        hidden = (sw * up_pre).astype(BF).astype(F32)
        route = jnp.sum(hidden * proj, axis=1, keepdims=True)
        gh = scaling * proj
        d1 = (gh * up_pre * sig * (1.0 + gate_pre * (1.0 - sig))).astype(BF)
        d2 = (gh * sw).astype(BF)
        deltas[at_chunk(h), 0:hid] = d1
        deltas[at_chunk(h), hid:] = d2
        scaleds[at_chunk(h), :] = (scaling * hidden).astype(BF)
        part = lax.dot_general(
            jnp.concatenate([d1, d2], axis=1), wab[...], (((1,), (1,)), ((), ())),
            preferred_element_type=F32)
        rp[h, :, :, 0:lw] = part.reshape(2, half, lw).astype(BF)
        rp[h, :, :, lw:] = jnp.broadcast_to(route, (chunk, LANES)).reshape(2, half, LANES).astype(BF)
        r1(h).start()
        return carry

    lax.fori_loop(0, n_hi, finish, 0)

    def r2(h):
        return rc(r2send.at[h], r2recv.at[hi], r2s.at[h], r2r.at[hi], ep=h * 2 + lo)

    def pair(h):
        r1(h).wait_recv()
        return rp[h, lo].astype(F32) + r1recv[h].astype(F32)

    def combine(i, carry):
        h = lax.rem(hi + i, n_hi)
        r2send[h] = pair(h).astype(BF)
        r2(h).start()
        return carry

    lax.fori_loop(1, n_hi, combine, 0)
    r2recv[hi] = pair(hi).astype(BF)

    tile = 256 if lw % 256 == 0 else 128

    def wgrad(i, carry):
        ds = pl.ds(pl.multiple_of(i * tile, LANES), tile)
        dn = (((0,), (0,)), ((), ()))
        both = lax.dot_general(xs[:, ds], deltas[...], dn, preferred_element_type=F32).astype(BF)
        ga[ds, :] = both[:, :hid]
        gb[ds, :] = both[:, hid:]
        gc[ds, :] = lax.dot_general(ys[:, ds], scaleds[...], dn, preferred_element_type=F32).astype(BF)
        return carry

    lax.fori_loop(0, lw // tile, wgrad, 0)
    outs = [
        pltpu.make_async_copy(ga, ga_hbm, w_sem.at[0]),
        pltpu.make_async_copy(gb, gb_hbm, w_sem.at[1]),
        pltpu.make_async_copy(gc, gc_hbm, w_sem.at[2]),
    ]
    for c in outs:
        c.start()

    for i in range(1, n_hi):
        h = lax.rem(hi + i, n_hi)
        rc(r2send.at[h], r2recv.at[h], r2s.at[h], r2r.at[h], ep=h * 2 + lo).wait_recv()
    for w in range(experts):
        acc = r2recv[w * per].astype(F32)
        for j in range(1, per):
            acc = acc + r2recv[w * per + j].astype(F32)
        retbuf[:, w] = acc.reshape(n_dp, CAP, lw + LANES).astype(BF)
    for j in range(1, n_dp):
        gp = lax.rem(g + j, n_dp)
        rc(retbuf.at[gp], fin.at[g], fs.at[j], fr.at[g], dp=gp).start()
    fin[g] = retbuf[g]
    for j in range(1, n_dp):
        gp = lax.rem(g + j, n_dp)
        rc(retbuf.at[gp], fin.at[gp], fs.at[j], fr.at[gp], dp=gp).wait_recv()

    for j in range(1, n_dp):
        gp = lax.rem(g + j, n_dp)
        slices(j, 0, gp).wait_send()
        slices(j, 1, gp).wait_send()
        rc(retbuf.at[gp], fin.at[g], fs.at[j], fr.at[g], dp=gp).wait_send()

    def drain(i, carry):
        h = lax.rem(hi + i, n_hi)
        for q in range(2):
            fwd(h % per, h // per, q).wait_send()
            onward(h % per, h // per, q, True)
        for b in range(nb):
            ar(b, h).wait_send()
        r1(h).wait_send()

        @pl.when(i >= 1)
        def _():
            r2(h).wait_send()
        return carry

    lax.fori_loop(0, n_hi, drain, 0)
    for i in range(1, experts):
        for q in range(2):
            across(i, q).wait_send()
    for c in outs:
        c.wait()


def finish_kernel(
    fin, sel_ref, ids_ref, ga_in, gb_in, gc_in, ig_hbm, rg_ref, ga_out, gb_out, gc_out,
    buf, obuf, sem_in, sem_out, osem,
):
    n_dp, experts, _, wide = fin.shape
    places = experts * CAP
    lw = wide - LANES
    rows = sel_ref.shape[0]
    stride = ROUTED // experts
    ins = [pltpu.make_async_copy(r, buf.at[i], sem_in.at[i]) for i, r in enumerate((ga_in, gb_in, gc_in))]
    outs = [pltpu.make_async_copy(buf.at[i], r, sem_out.at[i]) for i, r in enumerate((ga_out, gb_out, gc_out))]
    for c in ins:
        c.start()
    sel = sel_ref[...]
    selP = sel[:, :places].astype(BF)
    ocopies = []
    for j in range(n_dp):
        vals = fin[j].astype(F32).reshape(places, wide)
        obuf[:, j * lw:(j + 1) * lw] = jnp.dot(
            selP, vals[:, :lw].astype(BF), preferred_element_type=F32).astype(BF)
        ds = pl.ds(j * lw, lw)
        c = pltpu.make_async_copy(obuf.at[:, ds], ig_hbm.at[:, ds], osem.at[j])
        c.start()
        ocopies.append(c)
        if j < 3:
            ins[j].wait()
            outs[j].start()
    vals = fin[0].astype(F32).reshape(places, wide)
    route = jnp.concatenate([vals[:, lw:], jnp.zeros((LANES - places, LANES), F32)], axis=0).T[0:1]
    terms = sel * route
    pad = jnp.zeros((LANES - TOPK, rows), F32)
    ids = jnp.concatenate([ids_ref[...].astype(F32), pad], axis=0).T
    lane = lax.broadcasted_iota(jnp.int32, (rows, LANES), 1)
    wanted = jnp.where(lane < places, (lane // CAP) * stride, -1).astype(F32)
    rg = jnp.zeros((rows, LANES), F32)
    for k in range(TOPK):
        v = jnp.sum(jnp.where(ids[:, k:k + 1] == wanted, terms, 0.0), axis=1, keepdims=True)
        rg = jnp.where(lane == k, v, rg)
    rg_ref[...] = rg.T[:TOPK]
    for c in outs + ocopies:
        c.wait()


def body(tokens, out_grad, expert_ids, route_weights, gate_matrix, up_matrix, down_matrix):
    n_dp, n_ep = lax.axis_size("dp"), lax.axis_size("ep")
    experts = n_ep // SLICES
    n_hi = n_ep // 2
    rows, width = tokens.shape
    lw, hid = gate_matrix.shape
    nb = n_dp.bit_length() - 1
    chunk = 2 * n_dp * CAP
    half = n_dp * CAP
    total = n_hi * chunk
    C = 2 * lw + LANES
    R = lw + LANES
    V = pltpu.VMEM
    D = lambda *s: pltpu.SemaphoreType.DMA(s)
    anyspec = pl.BlockSpec(memory_space=pl.ANY)
    vspec = pl.BlockSpec(memory_space=pltpu.VMEM)
    ids = expert_ids.T
    grad = jax.ShapeDtypeStruct((lw, hid), BF)
    fin, sel, ga, gb, gc = pl.pallas_call(
        functools.partial(kernel, n_dp, n_ep),
        out_shape=(
            jax.ShapeDtypeStruct((n_dp, experts, CAP, R), BF),
            jax.ShapeDtypeStruct((rows, LANES), F32),
            grad, grad, grad,
        ),
        in_specs=[anyspec, anyspec, vspec, vspec, anyspec, anyspec, anyspec],
        out_specs=(vspec, vspec, anyspec, anyspec, anyspec),
        scratch_shapes=[
            V((n_dp, rows, lw), BF), V((n_dp, rows, lw), BF), V((lw, 2 * hid), BF), V((lw, hid), BF),
            V((n_dp, experts, CAP, C), BF), V((experts, n_dp, CAP, C), BF), V((n_ep, n_dp, CAP, C), BF),
            V((total, lw), BF), V((total, lw), BF), V((total, LANES), F32),
            V((n_hi, chunk, 3 * hid), F32), V((nb, n_hi, chunk, 3 * hid), BF), V((nb, n_hi, chunk, 3 * hid), BF),
            V((total, 2 * hid), BF), V((total, hid), BF),
            V((n_hi, 2, half, R), BF), V((n_hi, half, R), BF), V((n_hi, half, R), BF), V((n_hi, half, R), BF),
            V((n_dp, experts, CAP, R), BF),
            V((lw, hid), BF), V((lw, hid), BF), V((lw, hid), BF),
            D(2, n_dp), D(3), D(2, n_dp), D(2, n_dp), D(n_hi, 2), D(n_hi, 2), D(n_hi, 2), D(experts, 2),
            D(n_hi, 2), D(n_hi, 2),
            D(nb, n_hi), D(nb, n_hi), D(n_hi), D(n_hi), D(n_hi), D(n_hi), D(n_dp), D(n_dp),
        ],
        compiler_params=pltpu.CompilerParams(
            collective_id=0, has_side_effects=True, vmem_limit_bytes=67043328),
    )(tokens, out_grad, ids, route_weights.T, gate_matrix, up_matrix, down_matrix)
    ig, rg, ga, gb, gc = pl.pallas_call(
        finish_kernel,
        out_shape=(
            jax.ShapeDtypeStruct((rows, width), BF),
            jax.ShapeDtypeStruct((TOPK, rows), F32),
            grad, grad, grad,
        ),
        in_specs=[vspec, vspec, vspec, anyspec, anyspec, anyspec],
        out_specs=(anyspec, vspec, anyspec, anyspec, anyspec),
        scratch_shapes=[V((3, lw, hid), BF), V((rows, width), BF), D(3), D(3), D(n_dp)],
        compiler_params=pltpu.CompilerParams(vmem_limit_bytes=67043328),
    )(fin, sel, ids, ga, gb, gc)
    return ig, rg.T, ga, gb, gc


def solution(mesh):
    return jax.shard_map(
        body,
        mesh=mesh,
        in_specs=(
            P(("dp", "ep"), None),
            P(("dp", "ep"), None),
            P(("dp", "ep"), None),
            P(("dp", "ep"), None),
            P("dp", "ep"),
            P("dp", "ep"),
            P("dp", "ep"),
        ),
        out_specs=(
            P(("dp", "ep"), None),
            P(("dp", "ep"), None),
            P("dp", "ep"),
            P("dp", "ep"),
            P("dp", "ep"),
        ),
        check_vma=False,
    )
```

```python
import functools
import jax
import jax.numpy as jnp
from jax import lax
from jax.experimental import pallas as pl
from jax.experimental.pallas import tpu as pltpu
from jax.sharding import PartitionSpec as P

ROUTED = 256
TOPK = 8
SLICES = 8
CAP = 8
LANES = 128
BF = jnp.bfloat16
F32 = jnp.float32
MESH = pl.DeviceIdType.MESH


def kernel(
    n_dp, n_ep,
    tok_hbm, grad_hbm, ids_ref, rw_ref, a_hbm, b_hbm, c_hbm,
    fin, sel_ref, ga_hbm, gb_hbm, gc_hbm,
    tokbuf, gradbuf, wab, wc, send1, shard, ag, xs, ys, gates, psum, arsend, arrecv,
    deltas, scaleds, rp, r1recv, r2send, r2recv, retbuf, ga, gb, gc,
    in_sem, w_sem, s1s, s1r, s2s, s2d, s2r, sas, s3s, s3r, ars, arr, r1s, r1r, r2s, r2r, fs, fr,
):
    experts = n_ep // SLICES
    stride = ROUTED // experts
    places = experts * CAP
    n_hi = n_ep // 2
    rows, width = tok_hbm.shape
    lw, hid = a_hbm.shape
    nb = n_dp.bit_length() - 1
    chunk = 2 * n_dp * CAP
    half = n_dp * CAP
    g = lax.axis_index("dp")
    e = lax.axis_index("ep")
    hi, lo = e // 2, e % 2
    other = hi * 2 + (1 - lo)
    mine_w = e // SLICES

    def rc(src, dst, ss, rs, **where):
        return pltpu.make_async_remote_copy(
            src_ref=src, dst_ref=dst, send_sem=ss, recv_sem=rs,
            device_id=where, device_id_type=MESH)

    def cols(j):
        gp = lax.rem(g + j, n_dp)
        return gp, pl.ds(pl.multiple_of(gp * lw, LANES), lw)

    order = [n_dp // 2] + [j for j in range(1, n_dp) if j != n_dp // 2] + [0]
    loads = []
    for q, (src, buf) in enumerate(((tok_hbm, tokbuf), (grad_hbm, gradbuf))):
        for j in order:
            gp, ds = cols(j)
            c = pltpu.make_async_copy(src.at[:, ds], buf.at[j], in_sem.at[q, j])
            c.start()
            loads.append((q, j, gp, buf, c))
    wloads = [
        pltpu.make_async_copy(a_hbm, wab.at[:, pl.ds(0, hid)], w_sem.at[0]),
        pltpu.make_async_copy(b_hbm, wab.at[:, pl.ds(hid, hid)], w_sem.at[1]),
        pltpu.make_async_copy(c_hbm, wc, w_sem.at[2]),
    ]

    barrier = pltpu.get_barrier_semaphore()
    for j in range(1, n_dp):
        pl.semaphore_signal(barrier, inc=1, device_id={"dp": lax.rem(g + j, n_dp)}, device_id_type=MESH)
    for j in range(1, n_hi):
        pl.semaphore_signal(
            barrier, inc=1, device_id={"ep": lax.rem(hi + j, n_hi) * 2 + lo}, device_id_type=MESH)
    pl.semaphore_signal(barrier, inc=1, device_id={"ep": other}, device_id_type=MESH)

    pad = jnp.zeros((LANES - TOPK, rows), F32)
    ids = jnp.concatenate([ids_ref[...].astype(F32), pad], axis=0).T
    rw = jnp.concatenate([rw_ref[...].astype(F32), pad], axis=0).T
    lane = lax.broadcasted_iota(jnp.int32, (rows, LANES), 1)
    wanted = jnp.where(lane < places, (lane // CAP) * stride, -1).astype(F32)
    hits = jnp.zeros((rows, LANES), F32)
    wts = jnp.zeros((rows, LANES), F32)
    for k in range(TOPK):
        m = ids[:, k:k + 1] == wanted
        hits = hits + jnp.where(m, 1.0, 0.0)
        wts = wts + jnp.where(m, rw[:, k:k + 1], 0.0)
    tr = lax.broadcasted_iota(jnp.int32, (rows, rows), 0)
    tc = lax.broadcasted_iota(jnp.int32, (rows, rows), 1)
    lower = jnp.where(tc < tr, 1.0, 0.0).astype(BF)
    slot = jnp.dot(lower, hits.astype(BF), preferred_element_type=F32)
    sel = jnp.where(slot == (lane % CAP).astype(F32), hits, 0.0)
    sel_ref[...] = sel
    selT = sel.T[:places].astype(BF)
    gwT = (sel * wts).T[:places].astype(BF)
    gate = jnp.dot(gwT, jnp.ones((rows, LANES), BF), preferred_element_type=F32)
    gate = gate.reshape(experts, CAP, LANES).astype(BF)

    pl.semaphore_wait(barrier, n_dp - 1 + n_hi)

    pieces = (pl.ds(0, lw), pl.ds(lw, lw + LANES))

    def slices(j, q, gp):
        return rc(send1.at[j, :, :, pieces[q]], shard.at[:, g, :, pieces[q]], s1s.at[q, j], s1r.at[q, g], dp=gp)

    for q, j, gp, buf, c in loads:
        c.wait()
        r = jnp.dot(selT, buf[j], preferred_element_type=F32).reshape(experts, CAP, lw).astype(BF)
        if j:
            send1[j, :, :, q * lw:(q + 1) * lw] = r
            if q:
                send1[j, :, :, 2 * lw:] = gate
            slices(j, q, gp).start()
        else:
            shard[:, g, :, q * lw:(q + 1) * lw] = r
            if q:
                shard[:, g, :, 2 * lw:] = gate
    for c in wloads:
        c.start()

    per = SLICES // 2
    pos = hi % per
    base = hi - pos

    def at_order(k):
        m = jnp.where(pos < per - 1 - pos, pos, per - 1 - pos)
        near = jnp.where(k % 2 == 1, pos - (k + 1) // 2, pos + k // 2)
        far = jnp.where(pos < per - 1 - pos, k, per - 1 - k)
        return jnp.where(k <= 2 * m, near, far)

    def seen(h, q):
        return ag.at[h * 2 + lo, :, :, pieces[q]]

    def link(p, v, q, up):
        h = v * per + p
        to = hi + 1 - 2 * up
        return rc(seen(h, q), seen(h, q), (s2d if up else s2s).at[h, q], s2r.at[h, q], ep=to * 2 + lo)

    def link_in(p, v, q):
        h = v * per + p
        return rc(seen(h, q), seen(h, q), s2s.at[h, q], s2r.at[h, q], ep=other)

    def fwd(p, v, q):
        h = v * per + p
        return rc(seen(h, q), seen(h, q), s3s.at[h, q], s3r.at[h, q], ep=other)

    def fwd_in(p, v, q):
        h = v * per + p
        r = ag.at[h * 2 + 1 - lo, :, :, pieces[q]]
        return rc(r, r, s3s.at[h, q], s3r.at[h, q], ep=other)

    def across(i, q):
        h = lax.rem(hi + i * per, n_hi)
        return rc(shard.at[h // per, :, :, pieces[q]], seen(hi, q), sas.at[i, q], s2r.at[hi, q], ep=h * 2 + lo)

    def across_in(i, q):
        h = lax.rem(hi + i * per, n_hi)
        return rc(seen(h, q), seen(h, q), sas.at[i, q], s2r.at[h, q], ep=other)

    def onward(p, v, q, wait):
        @pl.when((p <= pos) & (pos < per - 1))
        def _():
            d = link(p, v, q, 0)
            d.wait_send() if wait else d.start()

        @pl.when((p >= pos) & (pos > 0))
        def _():
            d = link(p, v, q, 1)
            d.wait_send() if wait else d.start()

    for q in range(2):
        for j in range(1, n_dp):
            src = lax.rem(g + j, n_dp)
            rc(send1.at[j, :, :, pieces[q]], shard.at[:, src, :, pieces[q]], s1s.at[q, j], s1r.at[q, src], dp=src).wait_recv()
        for i in range(1, experts):
            across(i, q).start()
        if q:
            ag[e, :, :, lw:] = shard[mine_w, :, :, lw:]
        else:
            ag[e, :, :, :lw] = shard[mine_w, :, :, :lw]
        onward(pos, mine_w, q, False)
        fwd(pos, mine_w, q).start()
        for i in range(1, experts):
            across_in(i, q).wait_recv()
            v = lax.rem(mine_w + i, experts)
            onward(pos, v, q, False)
            fwd(pos, v, q).start()
    for c in wloads:
        c.wait()

    def ar(b, h):
        bit = 1 << b
        peer = g + (1 - 2 * ((g // bit) % 2)) * bit
        return rc(arsend.at[b, h], arrecv.at[b, h], ars.at[b, h], arr.at[b, h], dp=peer)

    def at_chunk(h):
        return pl.ds(pl.multiple_of(h * chunk, 16), chunk)

    def r1(h):
        return rc(rp.at[h, 1 - lo], r1recv.at[h], r1s.at[h], r1r.at[h], ep=other)

    def chunk_of(t):
        p, v = at_order(t // experts), t % experts
        return p, v, v * per + p

    def finish(i):
        p, v, h = chunk_of(i)
        ar(nb - 1, h).wait_recv()
        s = psum[h] + arrecv[nb - 1, h].astype(F32)
        gate_pre, up_pre, proj = s[:, :hid], s[:, hid:2 * hid], s[:, 2 * hid:]
        scaling = gates[at_chunk(h), 0:1]
        sig = 1.0 / (1.0 + jnp.exp(-gate_pre))
        sw = gate_pre * sig
        hidden = (sw * up_pre).astype(BF).astype(F32)
        route = jnp.sum(hidden * proj, axis=1, keepdims=True)
        gh = scaling * proj
        d1 = (gh * up_pre * sig * (1.0 + gate_pre * (1.0 - sig))).astype(BF)
        d2 = (gh * sw).astype(BF)
        deltas[at_chunk(h), 0:hid] = d1
        deltas[at_chunk(h), hid:] = d2
        scaleds[at_chunk(h), :] = (scaling * hidden).astype(BF)
        part = lax.dot_general(
            jnp.concatenate([d1, d2], axis=1), wab[...], (((1,), (1,)), ((), ())),
            preferred_element_type=F32)
        rp[h, :, :, 0:lw] = part.reshape(2, half, lw).astype(BF)
        rp[h, :, :, lw:] = jnp.broadcast_to(route, (chunk, LANES)).reshape(2, half, LANES).astype(BF)
        r1(h).start()

    def flow(t, carry):
        @pl.when((t >= experts) & (t < n_hi))
        def _():
            p, v, h = chunk_of(t)
            for q in range(2):
                link_in(p, v, q).wait_recv()
                onward(p, v, q, False)
                fwd(p, v, q).start()

        @pl.when((t >= 2) & (t <= n_hi + 1))
        def _():
            p, v, h = chunk_of(t - 2)
            fwd_in(p, v, 0).wait_recv()
            x = ag[pl.ds(h * 2, 2), :, :, 0:lw].astype(F32).reshape(chunk, lw).astype(BF)
            xs[at_chunk(h), :] = x
            p1 = jnp.dot(x, wab[...], preferred_element_type=F32)
            psum[h, :, 0:2 * hid] = p1
            arsend[0, h, :, 0:2 * hid] = p1.astype(BF)
            fwd_in(p, v, 1).wait_recv()
            y = ag[pl.ds(h * 2, 2), :, :, lw:2 * lw].astype(F32).reshape(chunk, lw).astype(BF)
            gates[at_chunk(h), :] = ag[pl.ds(h * 2, 2), :, :, 2 * lw:].astype(F32).reshape(chunk, LANES)
            ys[at_chunk(h), :] = y
            p2 = jnp.dot(y, wc[...], preferred_element_type=F32)
            psum[h, :, 2 * hid:] = p2
            arsend[0, h, :, 2 * hid:] = p2.astype(BF)
            ar(0, h).start()

        for b in range(nb - 1):
            @pl.when((t >= 3 + b) & (t < n_hi + 3 + b))
            def _(b=b):
                p, v, h = chunk_of(t - 3 - b)
                ar(b, h).wait_recv()
                s = psum[h] + arrecv[b, h].astype(F32)
                psum[h] = s
                arsend[b + 1, h] = s.astype(BF)
                ar(b + 1, h).start()

        @pl.when(t >= nb + 2)
        def _():
            finish(t - nb - 2)
        return carry

    lax.fori_loop(0, n_hi + nb + 2, flow, 0)

    def r2(h):
        return rc(r2send.at[h], r2recv.at[hi], r2s.at[h], r2r.at[hi], ep=h * 2 + lo)

    def pair(h):
        r1(h).wait_recv()
        return rp[h, lo].astype(F32) + r1recv[h].astype(F32)

    def combine(t, carry):
        p, v, h = chunk_of(t)
        both = pair(h).astype(BF)

        @pl.when(h != hi)
        def _():
            r2send[h] = both
            r2(h).start()

        @pl.when(h == hi)
        def _():
            r2recv[hi] = both
        return carry

    lax.fori_loop(0, n_hi, combine, 0)

    tile = 256 if lw % 256 == 0 else 128

    def wgrad(i, carry):
        ds = pl.ds(pl.multiple_of(i * tile, LANES), tile)
        dn = (((0,), (0,)), ((), ()))
        both = lax.dot_general(xs[:, ds], deltas[...], dn, preferred_element_type=F32).astype(BF)
        ga[ds, :] = both[:, :hid]
        gb[ds, :] = both[:, hid:]
        gc[ds, :] = lax.dot_general(ys[:, ds], scaleds[...], dn, preferred_element_type=F32).astype(BF)
        return carry

    lax.fori_loop(0, lw // tile, wgrad, 0)
    outs = [
        pltpu.make_async_copy(ga, ga_hbm, w_sem.at[0]),
        pltpu.make_async_copy(gb, gb_hbm, w_sem.at[1]),
        pltpu.make_async_copy(gc, gc_hbm, w_sem.at[2]),
    ]
    for c in outs:
        c.start()

    for i in range(1, n_hi):
        h = lax.rem(hi + i, n_hi)
        rc(r2send.at[h], r2recv.at[h], r2s.at[h], r2r.at[h], ep=h * 2 + lo).wait_recv()
    for w in range(experts):
        acc = r2recv[w * per].astype(F32)
        for j in range(1, per):
            acc = acc + r2recv[w * per + j].astype(F32)
        retbuf[:, w] = acc.reshape(n_dp, CAP, lw + LANES).astype(BF)
    for j in range(1, n_dp):
        gp = lax.rem(g + j, n_dp)
        rc(retbuf.at[gp], fin.at[g], fs.at[j], fr.at[g], dp=gp).start()
    fin[g] = retbuf[g]
    for j in range(1, n_dp):
        gp = lax.rem(g + j, n_dp)
        rc(retbuf.at[gp], fin.at[gp], fs.at[j], fr.at[gp], dp=gp).wait_recv()

    for j in range(1, n_dp):
        gp = lax.rem(g + j, n_dp)
        slices(j, 0, gp).wait_send()
        slices(j, 1, gp).wait_send()
        rc(retbuf.at[gp], fin.at[g], fs.at[j], fr.at[g], dp=gp).wait_send()

    def drain(i, carry):
        h = lax.rem(hi + i, n_hi)
        for q in range(2):
            fwd(h % per, h // per, q).wait_send()
            onward(h % per, h // per, q, True)
        for b in range(nb):
            ar(b, h).wait_send()
        r1(h).wait_send()

        @pl.when(i >= 1)
        def _():
            r2(h).wait_send()
        return carry

    lax.fori_loop(0, n_hi, drain, 0)
    for i in range(1, experts):
        for q in range(2):
            across(i, q).wait_send()
    for c in outs:
        c.wait()


def finish_kernel(
    fin, sel_ref, ids_ref, ga_in, gb_in, gc_in, ig_hbm, rg_ref, ga_out, gb_out, gc_out,
    buf, obuf, sem_in, sem_out, osem,
):
    n_dp, experts, _, wide = fin.shape
    places = experts * CAP
    lw = wide - LANES
    rows = sel_ref.shape[0]
    stride = ROUTED // experts
    ins = [pltpu.make_async_copy(r, buf.at[i], sem_in.at[i]) for i, r in enumerate((ga_in, gb_in, gc_in))]
    outs = [pltpu.make_async_copy(buf.at[i], r, sem_out.at[i]) for i, r in enumerate((ga_out, gb_out, gc_out))]
    for c in ins:
        c.start()
    sel = sel_ref[...]
    selP = sel[:, :places].astype(BF)
    for c, o in zip(ins, outs):
        c.wait()
        o.start()
    ocopies = []
    for j in range(n_dp):
        vals = fin[j].astype(F32).reshape(places, wide)
        obuf[:, j * lw:(j + 1) * lw] = jnp.dot(
            selP, vals[:, :lw].astype(BF), preferred_element_type=F32).astype(BF)
        ds = pl.ds(j * lw, lw)
        c = pltpu.make_async_copy(obuf.at[:, ds], ig_hbm.at[:, ds], osem.at[j])
        c.start()
        ocopies.append(c)
    vals = fin[0].astype(F32).reshape(places, wide)
    route = jnp.concatenate([vals[:, lw:], jnp.zeros((LANES - places, LANES), F32)], axis=0).T[0:1]
    terms = sel * route
    pad = jnp.zeros((LANES - TOPK, rows), F32)
    ids = jnp.concatenate([ids_ref[...].astype(F32), pad], axis=0).T
    lane = lax.broadcasted_iota(jnp.int32, (rows, LANES), 1)
    wanted = jnp.where(lane < places, (lane // CAP) * stride, -1).astype(F32)
    rg = jnp.zeros((rows, LANES), F32)
    for k in range(TOPK):
        v = jnp.sum(jnp.where(ids[:, k:k + 1] == wanted, terms, 0.0), axis=1, keepdims=True)
        rg = jnp.where(lane == k, v, rg)
    rg_ref[...] = rg.T[:TOPK]
    for c in outs + ocopies:
        c.wait()


def body(tokens, out_grad, expert_ids, route_weights, gate_matrix, up_matrix, down_matrix):
    n_dp, n_ep = lax.axis_size("dp"), lax.axis_size("ep")
    experts = n_ep // SLICES
    n_hi = n_ep // 2
    rows, width = tokens.shape
    lw, hid = gate_matrix.shape
    nb = n_dp.bit_length() - 1
    chunk = 2 * n_dp * CAP
    half = n_dp * CAP
    total = n_hi * chunk
    C = 2 * lw + LANES
    R = lw + LANES
    V = pltpu.VMEM
    D = lambda *s: pltpu.SemaphoreType.DMA(s)
    anyspec = pl.BlockSpec(memory_space=pl.ANY)
    vspec = pl.BlockSpec(memory_space=pltpu.VMEM)
    ids = expert_ids.T
    grad = jax.ShapeDtypeStruct((lw, hid), BF)
    fin, sel, ga, gb, gc = pl.pallas_call(
        functools.partial(kernel, n_dp, n_ep),
        out_shape=(
            jax.ShapeDtypeStruct((n_dp, experts, CAP, R), BF),
            jax.ShapeDtypeStruct((rows, LANES), F32),
            grad, grad, grad,
        ),
        in_specs=[anyspec, anyspec, vspec, vspec, anyspec, anyspec, anyspec],
        out_specs=(vspec, vspec, anyspec, anyspec, anyspec),
        scratch_shapes=[
            V((n_dp, rows, lw), BF), V((n_dp, rows, lw), BF), V((lw, 2 * hid), BF), V((lw, hid), BF),
            V((n_dp, experts, CAP, C), BF), V((experts, n_dp, CAP, C), BF), V((n_ep, n_dp, CAP, C), BF),
            V((total, lw), BF), V((total, lw), BF), V((total, LANES), F32),
            V((n_hi, chunk, 3 * hid), F32), V((nb, n_hi, chunk, 3 * hid), BF), V((nb, n_hi, chunk, 3 * hid), BF),
            V((total, 2 * hid), BF), V((total, hid), BF),
            V((n_hi, 2, half, R), BF), V((n_hi, half, R), BF), V((n_hi, half, R), BF), V((n_hi, half, R), BF),
            V((n_dp, experts, CAP, R), BF),
            V((lw, hid), BF), V((lw, hid), BF), V((lw, hid), BF),
            D(2, n_dp), D(3), D(2, n_dp), D(2, n_dp), D(n_hi, 2), D(n_hi, 2), D(n_hi, 2), D(experts, 2),
            D(n_hi, 2), D(n_hi, 2),
            D(nb, n_hi), D(nb, n_hi), D(n_hi), D(n_hi), D(n_hi), D(n_hi), D(n_dp), D(n_dp),
        ],
        compiler_params=pltpu.CompilerParams(
            collective_id=0, has_side_effects=True, vmem_limit_bytes=67043328),
    )(tokens, out_grad, ids, route_weights.T, gate_matrix, up_matrix, down_matrix)
    ig, rg, ga, gb, gc = pl.pallas_call(
        finish_kernel,
        out_shape=(
            jax.ShapeDtypeStruct((rows, width), BF),
            jax.ShapeDtypeStruct((TOPK, rows), F32),
            grad, grad, grad,
        ),
        in_specs=[vspec, vspec, vspec, anyspec, anyspec, anyspec],
        out_specs=(anyspec, vspec, anyspec, anyspec, anyspec),
        scratch_shapes=[V((3, lw, hid), BF), V((rows, width), BF), D(3), D(3), D(n_dp)],
        compiler_params=pltpu.CompilerParams(vmem_limit_bytes=67043328),
    )(fin, sel, ids, ga, gb, gc)
    return ig, rg.T, ga, gb, gc


def solution(mesh):
    return jax.shard_map(
        body,
        mesh=mesh,
        in_specs=(
            P(("dp", "ep"), None),
            P(("dp", "ep"), None),
            P(("dp", "ep"), None),
            P(("dp", "ep"), None),
            P("dp", "ep"),
            P("dp", "ep"),
            P("dp", "ep"),
        ),
        out_specs=(
            P(("dp", "ep"), None),
            P(("dp", "ep"), None),
            P("dp", "ep"),
            P("dp", "ep"),
            P("dp", "ep"),
        ),
        check_vma=False,
    )
```
